32 devices in a mesh: row: 8 (over z, y), col: 4 (over x, core).
Axes of the slice: x: 2, y: 2, z: 4, core: 2. Of those that a mesh axis runs over, the one named last changes fastest.
Arguments:
- eigvec_halves: float32 [1536, 32768], P('col', 'row'), may hold values from -6 to 6
- rotation_mate: int32 [1536], replicated, may hold values from 0 to 1535, as said below
- givens_theta: float32 [1536], replicated, may hold values from -3.140625 to 3.140625
- kept_vectors: int32 [1536], replicated, may hold values from 0 to 1535, as said below
- secular_singularities: float32 [1536], replicated, may hold values from -0.25 to 1535.25, as said below
- secular_coefficients: float32 [1536], replicated, may hold values from -6 to 6
- secular_zeros: float32 [512], replicated, may hold values from 0.4 to 1535.6, as said below
Outputs:
- packed_vectors: float32 [1536, 32768], P(('row', 'col'))
- panel: float32 [512, 32768], P('col', 'row')
The draws below stay inside these ranges and needn't reach their ends.
Inputs may be any that keep to these rules, and one draw needn't show every extreme that they name: `rotation_mate`: partner is an involution. Column blocks of 384 belong to the indices of col in order; at most 24 columns of one block pair with columns of any one other block, exactly that many for some two blocks in every draw. `kept_vectors`: survivors is a permutation. Compacted positions form consecutive blocks of 48, one block per device of row+col in order; one block takes at most 16 columns from any one column block of 384, exactly that many from some. secular_singularities[k] lies within 0.25 of k. secular_zeros[j] lies within 0.1 of an integer plus 0.5, between j * K / 512 and (j + 1) * K / 512.
All inputs are finite; a program needn't handle non-finite values.
Results may differ from the reference program's by a relative error of at most 0.00007.
Values sent between devices are 32-bit elements; how exact they have to be, the bound alone decides.
A program may use at most 128 MiB of HBM per device.

```python
import jax
import jax.numpy as jnp
from jax import lax

N = 32768
KD = 384
PANEL = 512
K = 1536
PAIR_CAP = 24
N_ROW = 8
N_COL = 4


def draw_rotation_mate(key, part):
    order_key, count_key = jax.random.split(jax.random.fold_in(key, 11))
    slot_order = jax.vmap(lambda subkey: jax.random.permutation(subkey, KD))(jax.random.split(order_key, N_COL)).astype(jnp.int32)
    counts = jax.random.randint(count_key, (N_COL, N_COL), PAIR_CAP // 2, PAIR_CAP + 1).astype(jnp.int32)
    counts = counts.at[1, 0].set(PAIR_CAP)
    device_ids = jnp.arange(N_COL, dtype=jnp.int32)[:, None]
    slot_ids = jnp.arange(N_COL * PAIR_CAP, dtype=jnp.int32)[None, :]
    round_ids = slot_ids // PAIR_CAP
    within = slot_ids % PAIR_CAP
    other_dev = (round_ids - device_ids) % N_COL
    limit = counts[round_ids, jnp.minimum(device_ids, other_dev)]
    twin_slot = within ^ 1
    same_dev = other_dev == device_ids
    active = jnp.where(same_dev, (within < limit) & (twin_slot < limit), within < limit)
    mate_slot = jnp.where(same_dev, round_ids * PAIR_CAP + twin_slot, slot_ids)
    mate_ids = other_dev * KD + slot_order[other_dev, mate_slot]
    local_labels = device_ids * KD + slot_order[device_ids, slot_ids]
    result = jnp.arange(K, dtype=jnp.int32)
    return result.at[local_labels.reshape(-1)].set(jnp.where(active, mate_ids, local_labels).reshape(-1))


def draw_kept_vectors(key, part):
    shift_key, own_key, place_key = jax.random.split(jax.random.fold_in(key, 23), 3)
    dest_count = N_ROW * N_COL
    every_destination = KD // N_ROW
    share_base = every_destination // N_COL
    share_extra = share_base // 3
    shifts = jax.random.permutation(shift_key, N_COL)[:2].astype(jnp.int32)
    source_ids = jnp.arange(N_COL, dtype=jnp.int32)[:, None]
    dest_ids = jnp.arange(dest_count, dtype=jnp.int32)[None, :]
    raised = ((source_ids + dest_ids + shifts[0]) % N_COL == 0).astype(jnp.int32)
    lowered = ((source_ids + dest_ids + shifts[1]) % N_COL == 0).astype(jnp.int32)
    load_table = share_base + share_extra * (raised - lowered)
    out_start = jnp.cumsum(load_table, axis=1) - load_table
    in_start = jnp.cumsum(load_table, axis=0) - load_table
    finish_table = in_start + load_table
    position_ids = jnp.arange(every_destination, dtype=jnp.int32)
    source_of = jnp.sum((finish_table.T[:, :, None] <= position_ids[None, None, :]).astype(jnp.int32), axis=1)
    offset_in = position_ids[None, :] - jnp.take_along_axis(in_start.T, source_of, axis=1)
    slot_here = jnp.take_along_axis(out_start.T, source_of, axis=1) + offset_in
    orders = jax.vmap(lambda subkey: jax.random.permutation(subkey, KD))(jax.random.split(own_key, N_COL)).astype(jnp.int32)
    column_ids = source_of * KD + orders[source_of, slot_here]
    shuffles = jax.vmap(lambda subkey: jax.random.permutation(subkey, every_destination))(jax.random.split(place_key, dest_count)).astype(jnp.int32)
    column_ids = jnp.take_along_axis(column_ids, shuffles, axis=1)
    return column_ids.reshape(-1).astype(jnp.int32)


def draw_secular_singularities(key, part):
    jitter_key = jax.random.fold_in(key, 31)
    base_ids = jnp.arange(K, dtype=jnp.float32)
    jitter = 0.1 * jnp.clip(jax.random.normal(jitter_key, (K,), jnp.float32), -2.5, 2.5)
    return base_ids + jitter


def draw_secular_zeros(key, part):
    placement_key, jitter_key = jax.random.split(jax.random.fold_in(key, 37))
    stride = K // PANEL
    offsets = jax.random.randint(placement_key, (PANEL,), 0, stride)
    centers = (jnp.arange(PANEL, dtype=jnp.int32) * stride + offsets).astype(jnp.float32) + 0.5
    jitter = 0.04 * jnp.clip(jax.random.normal(jitter_key, (PANEL,), jnp.float32), -2.5, 2.5)
    return centers + jitter


def shard_levels(rng, dims, cuts, low, high):
    def one(dim, shards_of):
        heights = jax.random.uniform(jax.random.fold_in(jax.random.fold_in(rng, 6), dim), (shards_of,), jnp.float32, low / len(cuts), high / len(cuts))
        return jnp.repeat(jnp.exp(heights), dims[dim] // shards_of).reshape((-1,) + (1,) * (len(dims) - dim - 1))

    gain = one(*cuts[0])
    for cut in cuts[1:]:
        gain = gain * one(*cut)
    return gain


def centred(key, extent, deviation, most, shards=(), held_as=jnp.bfloat16):
    values = deviation * jax.random.normal(key, extent, jnp.float32)
    if shards:
        values = values * shard_levels(key, extent, shards, -0.22, 0.18)
    return jnp.clip(values, -most, most).astype(held_as)


def setup_inputs(seed: int = 0) -> dict:
    seeds = jax.random.split(jax.random.key(seed), 8)
    return {
        "eigvec_halves": centred(seeds[0], (K, N), 1.0, 6.0, ((0, 4), (1, 8)), jnp.float32),
        "rotation_mate": draw_rotation_mate(jax.random.fold_in(seeds[7], 71), 0),
        "givens_theta": jnp.clip(jax.random.uniform(seeds[2], (K,), jnp.float32, -3.140625, 3.140625), -3.140625, 3.140625),
        "kept_vectors": draw_kept_vectors(jax.random.fold_in(seeds[7], 71), 0),
        "secular_singularities": draw_secular_singularities(jax.random.fold_in(seeds[7], 71), 0),
        "secular_coefficients": centred(seeds[5], (K,), 1.0, 6.0, (), jnp.float32),
        "secular_zeros": draw_secular_zeros(jax.random.fold_in(seeds[7], 71), 0),
    }


def reference(eigvec_halves, rotation_mate, givens_theta, kept_vectors, secular_singularities, secular_coefficients, secular_zeros):
    local_labels = jnp.arange(eigvec_halves.shape[0], dtype=jnp.int32)
    paired = rotation_mate != local_labels
    angles_here = givens_theta[jnp.minimum(local_labels, rotation_mate)]
    sign_flip = jnp.where(local_labels < rotation_mate, -1.0, 1.0).astype(jnp.float32)
    cosine = jnp.where(paired, jnp.cos(angles_here), 1.0)
    sine_term = jnp.where(paired, sign_flip * jnp.sin(angles_here), 0.0)
    spun_vectors = cosine[:, None] * eigvec_halves + sine_term[:, None] * eigvec_halves[rotation_mate]
    packed_vectors = spun_vectors[kept_vectors]
    cauchy_raw = secular_coefficients[:, None] / (secular_singularities[:, None] - secular_zeros[None, :])
    col_scale = lax.rsqrt(lax.optimization_barrier(jnp.sum(cauchy_raw * cauchy_raw, axis=0)) + 1e-06)
    cauchy = cauchy_raw * col_scale[None, :]
    panel = lax.dot_general(cauchy, packed_vectors, (((0,), (0,)), ((), ())), precision=lax.Precision.HIGHEST, preferred_element_type=jnp.float32)
    return (packed_vectors, panel)
```

```python
import functools

import jax
import jax.numpy as jnp
from jax import lax
from jax.experimental import pallas as pl
from jax.experimental.pallas import tpu as pltpu
from jax.sharding import PartitionSpec as P

MESH = pl.DeviceIdType.MESH
CHUNKS = 8
AHEAD = 2


def dot(a, b):
    return jnp.dot(a, b, precision=lax.Precision.HIGHEST, preferred_element_type=jnp.float32)


def rolled(array, shift, axis):
    twice = jnp.concatenate([array, array], axis=axis)
    return lax.dynamic_slice_in_dim(twice, shift, array.shape[axis], axis)


def exchange(
    rows, cols, width,
    x_ref, give_ref, own_ref, mate_ref, place_ref, weight_ref,
    packed_ref, panel_ref,
    rot_out, rot_in, col_out, col_in, row_out, half_out, half_in, half_own, part_out, part_in,
    rot_send, rot_recv, col_send, col_recv, row_send, row_recv, half_send, half_recv,
    part_send, part_recv, self_sem,
):
    row, col = lax.axis_index("row"), lax.axis_index("col")
    chips = cols // 2
    chip, core = col // 2, lax.rem(col, 2)
    twin = chip * 2 + 1 - core
    span = x_ref.shape[1]
    every = packed_ref.shape[0]
    cap = col_in.shape[2]
    blk = panel_ref.shape[0]

    barrier = pltpu.get_barrier_semaphore()
    for o in range(1, cols):
        pl.semaphore_signal(
            barrier, inc=1, device_id=(row, lax.rem(col + o, cols)), device_id_type=MESH
        )
    for q in range(1, rows):
        pl.semaphore_signal(
            barrier, inc=1, device_id=(lax.rem(row + q, rows), col), device_id_type=MESH
        )
    pl.semaphore_wait(barrier, cols + rows - 2)

    def lanes(c):
        return pl.ds(pl.multiple_of(c * width, 128), width)

    def rot_copy(c, o):
        return pltpu.make_async_remote_copy(
            rot_out.at[c, o - 1], rot_in.at[c, o - 1],
            rot_send.at[c, o - 1], rot_recv.at[c, o - 1],
            device_id=(row, lax.rem(col + o, cols)), device_id_type=MESH,
        )

    def col_copy(c, o):
        return pltpu.make_async_remote_copy(
            col_out.at[c, o - 1], col_in.at[c, o],
            col_send.at[c, o - 1], col_recv.at[c, o - 1],
            device_id=(row, lax.rem(col + o, cols)), device_id_type=MESH,
        )

    def target(c, source_row):
        return packed_ref.at[:, pl.ds(pl.multiple_of(source_row * span + c * width, 128), width)]

    def row_copy(c, q):
        return pltpu.make_async_remote_copy(
            row_out.at[c, q], target(c, row),
            row_send.at[c, q - 1], row_recv.at[c, q - 1],
            device_id=(lax.rem(row + q, rows), col), device_id_type=MESH,
        )

    def row_arrival(c, q):
        return pltpu.make_async_remote_copy(
            row_out.at[c, q], target(c, lax.rem(row + rows - q, rows)),
            row_send.at[c, q - 1], row_recv.at[c, q - 1],
            device_id=(lax.rem(row + q, rows), col), device_id_type=MESH,
        )

    def self_copy(c):
        return pltpu.make_async_copy(row_out.at[c, 0], target(c, row), self_sem.at[c])

    def half_copy(c):
        return pltpu.make_async_remote_copy(
            half_out.at[c], half_in.at[c], half_send.at[c], half_recv.at[c],
            device_id=(row, twin), device_id_type=MESH,
        )

    def part_copy(c, o):
        return pltpu.make_async_remote_copy(
            part_out.at[c, o - 1], part_in.at[c, o - 1],
            part_send.at[c, o - 1], part_recv.at[c, o - 1],
            device_id=(row, lax.rem(chip + o, chips) * 2 + core), device_id_type=MESH,
        )

    def send_mates(c):
        found = dot(give_ref[...], x_ref[:, lanes(c)])
        rot_out[c] = found.reshape(rot_out.shape[1:])
        for o in range(1, cols):
            rot_copy(c, o).start()

    def send_rows(c):
        for o in range(1, cols):
            col_copy(c, o).wait_recv()
        found = dot(place_ref[...], col_in[c].reshape(cols * cap, width))
        row_out[c] = found.reshape(rows, every, width)
        for q in range(1, rows):
            row_copy(c, q).start()
        self_copy(c).start()

    def fold(c):
        half_copy(c).wait_recv()
        total = half_own[c] + half_in[c]
        panel_ref[:, lanes(c)] = total[:blk]
        part_out[c] = total[blk:].reshape(chips - 1, blk, width)

    def main(c, carry):
        for o in range(1, cols):
            rot_copy(c, o).wait_recv()
        here = x_ref[:, lanes(c)]
        mates = rot_in[c].reshape(rot_in.shape[1] * rot_in.shape[2], width)
        spun = dot(own_ref[...], here) + dot(mate_ref[...], mates)
        col_in[c, 0] = spun[:cap]
        col_out[c] = spun[cap:].reshape(cols - 1, cap, width)
        for o in range(1, cols):
            col_copy(c, o).start()

        @pl.when(c + AHEAD < CHUNKS)
        def _():
            send_mates(c + AHEAD)

        sums = dot(weight_ref[...], here)
        half_own[c] = sums[: chips * blk]
        half_out[c] = sums[chips * blk :]
        half_copy(c).start()

        @pl.when(c >= 1)
        def _():
            fold(c - 1)

        @pl.when(c >= AHEAD)
        def _():
            send_rows(c - AHEAD)

        return carry

    lax.fori_loop(0, AHEAD, lambda c, z: (send_mates(c), z)[1], 0)
    lax.fori_loop(0, CHUNKS, main, 0)
    fold(CHUNKS - 1)

    def send_parts(c, carry):
        for o in range(1, chips):
            part_copy(c, o).start()
        return carry

    lax.fori_loop(0, CHUNKS, send_parts, 0)
    lax.fori_loop(CHUNKS - AHEAD, CHUNKS, lambda c, z: (send_rows(c), z)[1], 0)

    def finish_panel(c, carry):
        total = panel_ref[:, lanes(c)]
        for o in range(1, chips):
            part_copy(c, o).wait_recv()
            total = total + part_in[c, o - 1]
        panel_ref[:, lanes(c)] = total
        for o in range(1, chips):
            part_copy(c, o).wait_send()
        half_copy(c).wait_send()
        for o in range(1, cols):
            rot_copy(c, o).wait_send()
            col_copy(c, o).wait_send()
        return carry

    lax.fori_loop(0, CHUNKS, finish_panel, 0)

    def finish_rows(c, carry):
        for q in range(1, rows):
            row_arrival(c, q).wait_recv()
            row_copy(c, q).wait_send()
        self_copy(c).wait()
        return carry

    lax.fori_loop(0, CHUNKS, finish_rows, 0)


def shards(
    eigvec_halves,
    rotation_mate,
    givens_theta,
    kept_vectors,
    secular_singularities,
    secular_coefficients,
    secular_zeros,
):
    cols = lax.axis_size("col")
    rows = lax.axis_size("row")
    block, span = eigvec_halves.shape
    total_cols = rotation_mate.shape[0]
    panel_cols = secular_zeros.shape[0]
    pair_cap = block // 16
    chips = cols // 2
    blk = panel_cols // cols
    every = block // rows
    share = every // cols
    cap = rows * (share + share // 3)
    width = span // CHUNKS
    col, row = lax.axis_index("col"), lax.axis_index("row")
    first = col * block
    ids = jnp.arange(block, dtype=jnp.int32)
    labels = first + ids
    mate = lax.dynamic_slice_in_dim(rotation_mate, first, block)
    paired = mate != labels
    owner = mate // block
    remote = paired & (owner != col)

    def count(mask):
        return jnp.sum(mask.astype(jnp.int32), axis=0)

    same = (owner[:, None] == owner[None, :]) & remote[:, None]
    rank_out = count(same & (mate[:, None] < mate[None, :]))
    rank_in = count(same & (ids[:, None] < ids[None, :]))
    slot_out = jnp.where(remote, ((owner - col + cols) % cols - 1) * pair_cap + rank_out, -1)
    slot_in = jnp.where(remote, ((col - owner + cols) % cols - 1) * pair_cap + rank_in, -1)
    pair_slots = jnp.arange((cols - 1) * pair_cap, dtype=jnp.int32)
    give = (pair_slots[:, None] == slot_out[None, :]).astype(jnp.float32)

    every_id = jnp.arange(total_cols, dtype=jnp.int32)

    def lookup(mask, values):
        return jnp.sum(jnp.where(mask, values[:, None], jnp.zeros((), values.dtype)), axis=0)

    mine = kept_vectors[:, None] == labels[None, :]
    theirs = kept_vectors[:, None] == mate[None, :]
    spot, spot_mate = lookup(mine, every_id), lookup(theirs, every_id)
    pole, pole_mate = lookup(mine, secular_singularities), lookup(theirs, secular_singularities)
    weight, weight_mate = lookup(mine, secular_coefficients), lookup(theirs, secular_coefficients)
    angle = lookup(every_id[:, None] == jnp.minimum(labels, mate)[None, :], givens_theta)
    cosine = jnp.where(paired, jnp.cos(angle), 1.0)
    sine = jnp.where(paired, jnp.where(labels < mate, -1.0, 1.0) * jnp.sin(angle), 0.0)

    goal, goal_mate = (spot // every) % cols, (spot_mate // every) % cols

    def move_slot(goals, spots):
        before = (goal[:, None] == goals[None, :]) & (spot[:, None] < spots[None, :])
        return ((goals - col + cols) % cols) * cap + count(before)

    slot, slot_mate = move_slot(goal, spot), move_slot(goal_mate, spot_mate)
    move_slots = jnp.arange(cols * cap, dtype=jnp.int32)
    local = paired & jnp.logical_not(remote)
    own = jnp.where(move_slots[:, None] == slot[None, :], cosine[None, :], 0.0) + jnp.where(
        (move_slots[:, None] == slot_mate[None, :]) & local[None, :], -sine[None, :], 0.0
    )
    taken = slot_in[:, None] == pair_slots[None, :]
    from_slot, from_sine = lookup(taken, slot), lookup(taken, sine)
    from_mate = jnp.where(move_slots[:, None] == from_slot[None, :], from_sine[None, :], 0.0)

    wanted = lax.dynamic_index_in_dim(
        kept_vectors.reshape(rows, cols, every), col, 1, keepdims=False
    ).reshape(-1)
    source = wanted // block
    rank = count((source[:, None] == source[None, :]) & (ids[:, None] < ids[None, :]))
    arrived = ((col - source + cols) % cols) * cap + rank
    arrived = rolled(arrived.reshape(rows, every), row, 0).reshape(-1)
    place = (arrived[:, None] == move_slots[None, :]).astype(jnp.float32)

    raw = secular_coefficients[:, None] / (
        secular_singularities[:, None] - secular_zeros[None, :]
    )
    scale = lax.rsqrt(jnp.sum(raw * raw, axis=0) + 1e-06)

    def ordered(array):
        parts = rolled(array.reshape(chips, 2, blk), col // 2, 0)
        return rolled(parts, col % 2, 1).transpose(1, 0, 2).reshape(-1)

    zeros, scale = ordered(secular_zeros), ordered(scale)
    cauchy = weight[None, :] / (pole[None, :] - zeros[:, None])
    cauchy_mate = weight_mate[None, :] / (pole_mate[None, :] - zeros[:, None])
    weights = (cosine[None, :] * cauchy - sine[None, :] * cauchy_mate) * scale[:, None]

    vmem = pl.BlockSpec(memory_space=pltpu.VMEM)
    f32 = jnp.float32
    dma = pltpu.SemaphoreType.DMA
    return pl.pallas_call(
        functools.partial(exchange, rows, cols, width),
        out_shape=(
            jax.ShapeDtypeStruct((every, rows * span), f32),
            jax.ShapeDtypeStruct((blk, span), f32),
        ),
        in_specs=[vmem] * 6,
        out_specs=(pl.BlockSpec(memory_space=pl.ANY), vmem),
        scratch_shapes=[
            pltpu.VMEM((CHUNKS, cols - 1, pair_cap, width), f32),
            pltpu.VMEM((CHUNKS, cols - 1, pair_cap, width), f32),
            pltpu.VMEM((CHUNKS, cols - 1, cap, width), f32),
            pltpu.VMEM((CHUNKS, cols, cap, width), f32),
            pltpu.VMEM((CHUNKS, rows, every, width), f32),
            pltpu.VMEM((CHUNKS, chips * blk, width), f32),
            pltpu.VMEM((CHUNKS, chips * blk, width), f32),
            pltpu.VMEM((CHUNKS, chips * blk, width), f32),
            pltpu.VMEM((CHUNKS, chips - 1, blk, width), f32),
            pltpu.VMEM((CHUNKS, chips - 1, blk, width), f32),
            dma((CHUNKS, cols - 1)), dma((CHUNKS, cols - 1)),
            dma((CHUNKS, cols - 1)), dma((CHUNKS, cols - 1)),
            dma((CHUNKS, rows - 1)), dma((CHUNKS, rows - 1)),
            dma((CHUNKS,)), dma((CHUNKS,)),
            dma((CHUNKS, chips - 1)), dma((CHUNKS, chips - 1)),
            dma((CHUNKS,)),
        ],
        compiler_params=pltpu.CompilerParams(
            collective_id=0, has_side_effects=True, vmem_limit_bytes=60 * 1024 * 1024
        ),
    )(eigvec_halves, give, own, from_mate, place, weights)


def solution(mesh):
    placed = (P("col", "row"), P(), P(), P(), P(), P(), P())
    return jax.shard_map(
        shards,
        mesh=mesh,
        in_specs=placed,
        out_specs=(P(("row", "col"), None), P("col", "row")),
        check_vma=False,
    )
```

```python
import functools

import jax
import jax.numpy as jnp
from jax import lax
from jax.experimental import pallas as pl
from jax.experimental.pallas import tpu as pltpu
from jax.sharding import PartitionSpec as P

MESH = pl.DeviceIdType.MESH
CHUNKS = 16
AHEAD = 2


def dot(a, b):
    return jnp.dot(a, b, precision=lax.Precision.HIGHEST, preferred_element_type=jnp.float32)


def rolled(array, shift, axis):
    twice = jnp.concatenate([array, array], axis=axis)
    return lax.dynamic_slice_in_dim(twice, shift, array.shape[axis], axis)


def exchange(
    rows, cols, width,
    x_ref, give_ref, own_ref, mate_ref, place_ref, weight_ref,
    packed_ref, panel_ref,
    rot_out, rot_in, col_out, col_in, row_out, half_out, half_in, half_own, part_out, part_in,
    rot_send, rot_recv, col_send, col_recv, row_send, row_recv, half_send, half_recv,
    part_send, part_recv, self_sem,
):
    row, col = lax.axis_index("row"), lax.axis_index("col")
    chips = cols // 2
    chip, core = col // 2, lax.rem(col, 2)
    twin = chip * 2 + 1 - core
    span = x_ref.shape[1]
    every = packed_ref.shape[0]
    cap = col_in.shape[2]
    blk = panel_ref.shape[0]

    barrier = pltpu.get_barrier_semaphore()
    for o in range(1, cols):
        pl.semaphore_signal(
            barrier, inc=1, device_id=(row, lax.rem(col + o, cols)), device_id_type=MESH
        )
    for q in range(1, rows):
        pl.semaphore_signal(
            barrier, inc=1, device_id=(lax.rem(row + q, rows), col), device_id_type=MESH
        )
    pl.semaphore_wait(barrier, cols + rows - 2)

    def lanes(c):
        return pl.ds(pl.multiple_of(c * width, 128), width)

    def rot_copy(c, o):
        return pltpu.make_async_remote_copy(
            rot_out.at[c, o - 1], rot_in.at[c, o - 1],
            rot_send.at[c, o - 1], rot_recv.at[c, o - 1],
            device_id=(row, lax.rem(col + o, cols)), device_id_type=MESH,
        )

    def col_copy(c, o):
        return pltpu.make_async_remote_copy(
            col_out.at[c, o - 1], col_in.at[c, o],
            col_send.at[c, o - 1], col_recv.at[c, o - 1],
            device_id=(row, lax.rem(col + o, cols)), device_id_type=MESH,
        )

    def target(c, source_row):
        return packed_ref.at[:, pl.ds(pl.multiple_of(source_row * span + c * width, 128), width)]

    def row_copy(c, q):
        return pltpu.make_async_remote_copy(
            row_out.at[c, q], target(c, row),
            row_send.at[c, q - 1], row_recv.at[c, q - 1],
            device_id=(lax.rem(row + q, rows), col), device_id_type=MESH,
        )

    def row_arrival(c, q):
        return pltpu.make_async_remote_copy(
            row_out.at[c, q], target(c, lax.rem(row + rows - q, rows)),
            row_send.at[c, q - 1], row_recv.at[c, q - 1],
            device_id=(lax.rem(row + q, rows), col), device_id_type=MESH,
        )

    def self_copy(c):
        return pltpu.make_async_copy(row_out.at[c, 0], target(c, row), self_sem.at[c])

    def half_copy(c):
        return pltpu.make_async_remote_copy(
            half_out.at[c], half_in.at[c], half_send.at[c], half_recv.at[c],
            device_id=(row, twin), device_id_type=MESH,
        )

    def part_copy(c, o):
        return pltpu.make_async_remote_copy(
            part_out.at[c, o - 1], part_in.at[c, o - 1],
            part_send.at[c, o - 1], part_recv.at[c, o - 1],
            device_id=(row, lax.rem(chip + o, chips) * 2 + core), device_id_type=MESH,
        )

    def send_mates(c):
        found = dot(give_ref[...], x_ref[:, lanes(c)])
        rot_out[c] = found.reshape(rot_out.shape[1:])
        for o in range(1, cols):
            rot_copy(c, o).start()

    def send_rows(c):
        for o in range(1, cols):
            col_copy(c, o).wait_recv()
        found = dot(place_ref[...], col_in[c].reshape(cols * cap, width))
        row_out[c] = found.reshape(rows, every, width)
        for q in range(1, rows):
            row_copy(c, q).start()
        self_copy(c).start()

    def fold(c):
        half_copy(c).wait_recv()
        total = half_own[c] + half_in[c]
        panel_ref[:, lanes(c)] = total[:blk]
        part_out[c] = total[blk:].reshape(chips - 1, blk, width)

    def main(c, carry):
        for o in range(1, cols):
            rot_copy(c, o).wait_recv()
        here = x_ref[:, lanes(c)]
        mates = rot_in[c].reshape(rot_in.shape[1] * rot_in.shape[2], width)
        spun = dot(own_ref[...], here) + dot(mate_ref[...], mates)
        col_in[c, 0] = spun[:cap]
        col_out[c] = spun[cap:].reshape(cols - 1, cap, width)
        for o in range(1, cols):
            col_copy(c, o).start()

        @pl.when(c + AHEAD < CHUNKS)
        def _():
            send_mates(c + AHEAD)

        @pl.when(c >= AHEAD)
        def _():
            send_rows(c - AHEAD)

        sums = dot(weight_ref[...], here)
        half_own[c] = sums[: chips * blk]
        half_out[c] = sums[chips * blk :]
        half_copy(c).start()

        @pl.when(c >= 1)
        def _():
            fold(c - 1)

        return carry

    lax.fori_loop(0, AHEAD, lambda c, z: (send_mates(c), z)[1], 0)
    lax.fori_loop(0, CHUNKS, main, 0)
    fold(CHUNKS - 1)

    def send_parts(c, carry):
        for o in range(1, chips):
            part_copy(c, o).start()
        return carry

    lax.fori_loop(0, CHUNKS, send_parts, 0)
    lax.fori_loop(CHUNKS - AHEAD, CHUNKS, lambda c, z: (send_rows(c), z)[1], 0)

    def finish_panel(c, carry):
        total = panel_ref[:, lanes(c)]
        for o in range(1, chips):
            part_copy(c, o).wait_recv()
            total = total + part_in[c, o - 1]
        panel_ref[:, lanes(c)] = total
        for o in range(1, chips):
            part_copy(c, o).wait_send()
        half_copy(c).wait_send()
        for o in range(1, cols):
            rot_copy(c, o).wait_send()
            col_copy(c, o).wait_send()
        return carry

    lax.fori_loop(0, CHUNKS, finish_panel, 0)

    def finish_rows(c, carry):
        for q in range(1, rows):
            row_arrival(c, q).wait_recv()
            row_copy(c, q).wait_send()
        self_copy(c).wait()
        return carry

    lax.fori_loop(0, CHUNKS, finish_rows, 0)


def shards(
    eigvec_halves,
    rotation_mate,
    givens_theta,
    kept_vectors,
    secular_singularities,
    secular_coefficients,
    secular_zeros,
):
    cols = lax.axis_size("col")
    rows = lax.axis_size("row")
    block, span = eigvec_halves.shape
    total_cols = rotation_mate.shape[0]
    panel_cols = secular_zeros.shape[0]
    pair_cap = block // 16
    chips = cols // 2
    blk = panel_cols // cols
    every = block // rows
    share = every // cols
    cap = rows * (share + share // 3)
    width = span // CHUNKS
    col, row = lax.axis_index("col"), lax.axis_index("row")
    first = col * block
    ids = jnp.arange(block, dtype=jnp.int32)
    labels = first + ids
    mate = lax.dynamic_slice_in_dim(rotation_mate, first, block)
    paired = mate != labels
    owner = mate // block
    remote = paired & (owner != col)

    def count(mask):
        return jnp.sum(mask.astype(jnp.int32), axis=0)

    same = (owner[:, None] == owner[None, :]) & remote[:, None]
    rank_out = count(same & (mate[:, None] < mate[None, :]))
    rank_in = count(same & (ids[:, None] < ids[None, :]))
    slot_out = jnp.where(remote, ((owner - col + cols) % cols - 1) * pair_cap + rank_out, -1)
    slot_in = jnp.where(remote, ((col - owner + cols) % cols - 1) * pair_cap + rank_in, -1)
    pair_slots = jnp.arange((cols - 1) * pair_cap, dtype=jnp.int32)
    give = (pair_slots[:, None] == slot_out[None, :]).astype(jnp.float32)

    every_id = jnp.arange(total_cols, dtype=jnp.int32)

    def lookup(mask, values):
        return jnp.sum(jnp.where(mask, values[:, None], jnp.zeros((), values.dtype)), axis=0)

    mine = kept_vectors[:, None] == labels[None, :]
    theirs = kept_vectors[:, None] == mate[None, :]
    spot, spot_mate = lookup(mine, every_id), lookup(theirs, every_id)
    pole, pole_mate = lookup(mine, secular_singularities), lookup(theirs, secular_singularities)
    weight, weight_mate = lookup(mine, secular_coefficients), lookup(theirs, secular_coefficients)
    angle = lookup(every_id[:, None] == jnp.minimum(labels, mate)[None, :], givens_theta)
    cosine = jnp.where(paired, jnp.cos(angle), 1.0)
    sine = jnp.where(paired, jnp.where(labels < mate, -1.0, 1.0) * jnp.sin(angle), 0.0)

    goal, goal_mate = (spot // every) % cols, (spot_mate // every) % cols

    def move_slot(goals, spots):
        before = (goal[:, None] == goals[None, :]) & (spot[:, None] < spots[None, :])
        return ((goals - col + cols) % cols) * cap + count(before)

    slot, slot_mate = move_slot(goal, spot), move_slot(goal_mate, spot_mate)
    move_slots = jnp.arange(cols * cap, dtype=jnp.int32)
    local = paired & jnp.logical_not(remote)
    own = jnp.where(move_slots[:, None] == slot[None, :], cosine[None, :], 0.0) + jnp.where(
        (move_slots[:, None] == slot_mate[None, :]) & local[None, :], -sine[None, :], 0.0
    )
    taken = slot_in[:, None] == pair_slots[None, :]
    from_slot, from_sine = lookup(taken, slot), lookup(taken, sine)
    from_mate = jnp.where(move_slots[:, None] == from_slot[None, :], from_sine[None, :], 0.0)

    wanted = lax.dynamic_index_in_dim(
        kept_vectors.reshape(rows, cols, every), col, 1, keepdims=False
    ).reshape(-1)
    source = wanted // block
    rank = count((source[:, None] == source[None, :]) & (ids[:, None] < ids[None, :]))
    arrived = ((col - source + cols) % cols) * cap + rank
    arrived = rolled(arrived.reshape(rows, every), row, 0).reshape(-1)
    place = (arrived[:, None] == move_slots[None, :]).astype(jnp.float32)

    raw = secular_coefficients[:, None] / (
        secular_singularities[:, None] - secular_zeros[None, :]
    )
    scale = lax.rsqrt(jnp.sum(raw * raw, axis=0) + 1e-06)

    def ordered(array):
        parts = rolled(array.reshape(chips, 2, blk), col // 2, 0)
        return rolled(parts, col % 2, 1).transpose(1, 0, 2).reshape(-1)

    zeros, scale = ordered(secular_zeros), ordered(scale)
    cauchy = weight[None, :] / (pole[None, :] - zeros[:, None])
    cauchy_mate = weight_mate[None, :] / (pole_mate[None, :] - zeros[:, None])
    weights = (cosine[None, :] * cauchy - sine[None, :] * cauchy_mate) * scale[:, None]

    vmem = pl.BlockSpec(memory_space=pltpu.VMEM)
    f32 = jnp.float32
    dma = pltpu.SemaphoreType.DMA
    return pl.pallas_call(
        functools.partial(exchange, rows, cols, width),
        out_shape=(
            pltpu.VMEM((every, rows * span), f32),
            pltpu.VMEM((blk, span), f32),
        ),
        in_specs=[vmem] * 6,
        out_specs=(vmem, vmem),
        scratch_shapes=[
            pltpu.VMEM((CHUNKS, cols - 1, pair_cap, width), f32),
            pltpu.VMEM((CHUNKS, cols - 1, pair_cap, width), f32),
            pltpu.VMEM((CHUNKS, cols - 1, cap, width), f32),
            pltpu.VMEM((CHUNKS, cols, cap, width), f32),
            pltpu.VMEM((CHUNKS, rows, every, width), f32),
            pltpu.VMEM((CHUNKS, chips * blk, width), f32),
            pltpu.VMEM((CHUNKS, chips * blk, width), f32),
            pltpu.VMEM((CHUNKS, chips * blk, width), f32),
            pltpu.VMEM((CHUNKS, chips - 1, blk, width), f32),
            pltpu.VMEM((CHUNKS, chips - 1, blk, width), f32),
            dma((CHUNKS, cols - 1)), dma((CHUNKS, cols - 1)),
            dma((CHUNKS, cols - 1)), dma((CHUNKS, cols - 1)),
            dma((CHUNKS, rows - 1)), dma((CHUNKS, rows - 1)),
            dma((CHUNKS,)), dma((CHUNKS,)),
            dma((CHUNKS, chips - 1)), dma((CHUNKS, chips - 1)),
            dma((CHUNKS,)),
        ],
        compiler_params=pltpu.CompilerParams(
            collective_id=0, has_side_effects=True, vmem_limit_bytes=54 * 1024 * 1024
        ),
    )(eigvec_halves, give, own, from_mate, place, weights)


def solution(mesh):
    placed = (P("col", "row"), P(), P(), P(), P(), P(), P())
    return jax.shard_map(
        shards,
        mesh=mesh,
        in_specs=placed,
        out_specs=(P(("row", "col"), None), P("col", "row")),
        check_vma=False,
    )
```
